32 devices in a mesh: req: 8 (over z, x), seq: 4 (over y, core).
Axes of the slice: x: 2, y: 2, z: 4, core: 2. Of those that a mesh axis runs over, the one named last changes fastest.
Arguments:
- pool_states: float32 [104, 64, 64, 128], P('req', 'seq'), may hold values from -6 to 6
- inner_window: bfloat16 [104, 3, 4096], P('req', None, 'seq'), may hold values from -6 to 6
- state_window: bfloat16 [104, 3, 256], P('req', None, 'seq'), may hold values from -6 to 6
- move_plan: int32 [104, 2], P('req'), may hold values from 0 to 12, as said below
- active_mask: int32 [104], P('req'), may hold values 0 or 1
- inputs_inner: bfloat16 [8, 2048, 4096], P('req', 'seq'), may hold values from -6 to 6
- inputs_state: bfloat16 [8, 2048, 256], P('req', 'seq'), may hold values from -6 to 6
- gate_rows: bfloat16 [8, 2048, 4096], P('req', 'seq'), may hold values from -6 to 6
- step_raw: bfloat16 [8, 2048, 64], P('req', 'seq'), may hold values from -8 to 60
- lengths: int32 [8], P('req'), may hold values from 4 to 2048
- conv_weight: float32 [4, 4352], replicated, may hold values from -3 to 3
- conv_bias: float32 [4352], replicated, may hold values from -3 to 3
- step_bias: float32 [64], replicated, may hold values from -3.3 to -2.7
- decay_log: float32 [64], replicated, may hold values from -10 to 0
- skip_weight: float32 [64], replicated, may hold values from 0.5 to 1.5
- norm_weight: float32 [4096], replicated, may hold values from 0.25 to 1.75
Outputs:
- new_states: float32 [104, 64, 64, 128], P('req', 'seq')
- new_inner_window: bfloat16 [104, 3, 4096], P('req', None, 'seq')
- new_state_window: bfloat16 [104, 3, 256], P('req', None, 'seq')
- mixer_out: bfloat16 [8, 2048, 4096], P('req', 'seq')
The draws below stay inside these ranges and needn't reach their ends.
Inputs may be any that keep to these rules, and one draw needn't show every extreme that they name: `move_plan`: every pair of a destination index along req and a slot 0 .. 12 is named exactly once; the rows of one device name one destination at most 4 times, and some destination exactly 4 times.
All inputs are finite; a program needn't handle non-finite values. No bound on the sum of `active_mask` on one device may be relied on, other than what follows from the above.
Results may differ from the reference program's by a relative error of at most 0.0087.
Values may be sent and summed in bfloat16 or wider, within the bound.
A program may use at most 192 MiB of HBM per device.

```python
import jax
import jax.numpy as jnp
from jax import lax

HEAD_COUNT = 64
HEAD_DIM = 64
STATE_DIM = 128
KERNEL = 4
BLOCK_LEN = 256
SLOTS_DEV = 13
PREFILLS = 1
INNER_DIM = 4096
CHANNELS = 4352
CAPACITY = 4
PROMPT_SPAN = 2048
PROMPT_TOTAL = 8
POOL_SLOTS = 104


def draw_move_plan(key, part):
    peer_count = POOL_SLOTS // SLOTS_DEV
    sampler_seeds = jax.random.split(jax.random.fold_in(key, 11), 5)
    outer_order = jax.random.permutation(sampler_seeds[0], peer_count)
    inner_order = jax.random.permutation(sampler_seeds[1], peer_count)
    slot_order = jax.random.permutation(sampler_seeds[2], SLOTS_DEV)
    rotation = jax.random.randint(sampler_seeds[3], (), 0, peer_count)
    offsets = ((jnp.arange(SLOTS_DEV) // CAPACITY + rotation) % peer_count)[slot_order]
    devices = jnp.arange(peer_count)
    target_device = outer_order[(inner_order[devices][:, None] + offsets[None, :]) % peer_count]

    def slot_table(table_key):
        return jax.random.permutation(table_key, SLOTS_DEV)
    slot_tables = jax.vmap(slot_table)(jax.random.split(sampler_seeds[4], peer_count))
    target_slot = slot_tables[target_device, jnp.arange(SLOTS_DEV)[None, :]]
    return jnp.stack([target_device, target_slot], axis=-1).reshape(POOL_SLOTS, 2).astype(jnp.int32)


def draw_step_raw(key, part):
    sampler_seeds = jax.random.split(jax.random.fold_in(key, 23), 4)
    blocks = PROMPT_SPAN // BLOCK_LEN
    offset_steps = jax.random.uniform(sampler_seeds[0], (PROMPT_TOTAL, blocks, 1, HEAD_COUNT), minval=-0.8, maxval=0.8)
    offset_steps = jnp.broadcast_to(offset_steps, (PROMPT_TOTAL, blocks, BLOCK_LEN, HEAD_COUNT)).reshape(PROMPT_TOTAL, PROMPT_SPAN, HEAD_COUNT)
    jitter_addend = 0.7 * jax.random.normal(sampler_seeds[1], (PROMPT_TOTAL, PROMPT_SPAN, HEAD_COUNT))
    arrival_tallies = jax.random.uniform(sampler_seeds[2], (PROMPT_TOTAL, PROMPT_SPAN, 1)) < 3.0 / PROMPT_SPAN
    level_entries = jax.random.uniform(sampler_seeds[3], (PROMPT_TOTAL, PROMPT_SPAN, HEAD_COUNT), minval=34.0, maxval=46.0)
    payload_array = offset_steps + jitter_addend + jnp.where(arrival_tallies, level_entries, 0.0)
    return jnp.clip(payload_array, -8.0, 60.0).astype(jnp.float32).astype(jnp.bfloat16)


def draw_decay_log(key, part):
    sampler_seeds = jax.random.split(jax.random.fold_in(key, 37), 3)
    slow_low = jnp.log(0.5 / (0.05 * PROMPT_SPAN))
    slow_high = jnp.log(2.0 / (0.05 * PROMPT_SPAN))
    fast_share = 0.5
    slow_part = jax.random.uniform(sampler_seeds[0], (HEAD_COUNT,), minval=slow_low, maxval=slow_high)
    fast_part = jax.random.uniform(sampler_seeds[1], (HEAD_COUNT,), minval=jnp.log(0.3), maxval=jnp.log(0.67))
    fast_pick = jax.random.uniform(sampler_seeds[2], (HEAD_COUNT,)) < fast_share
    return jnp.where(fast_pick, fast_part, slow_part).astype(jnp.float32)


def plant(drawn, stream_key, low, largest):
    longest = drawn.shape.index(max(drawn.shape))
    spots = []
    for shift in (0, 1):
        where = [jax.random.randint(jax.random.fold_in(stream_key, axis), (), 0, length) for axis, length in enumerate(drawn.shape)]
        where[longest] = (where[longest] + shift) % drawn.shape[longest]
        spots.append(tuple(where))
    return drawn.at[spots[0]].set(low).at[spots[1]].set(largest)


def block_scale(own_key, shape, shards, least, high):
    level = 1.0
    for dim, blocks in shards:
        draws = jax.random.uniform(jax.random.fold_in(jax.random.fold_in(own_key, 6), dim), (blocks,), jnp.float32, least / len(shards), high / len(shards))
        level = level * jnp.repeat(jnp.exp(draws), shape[dim] // blocks).reshape((-1,) + (1,) * (len(shape) - 1 - dim))
    return level


def normal_values(own_key, dims, width, limit, pieces=(), kind=jnp.bfloat16):
    entries = jax.random.normal(own_key, dims, jnp.float32) * width
    if len(pieces) > 0:
        entries = block_scale(own_key, dims, pieces, -0.22, 0.18) * entries
    return jnp.clip(entries, min=-limit, max=limit).astype(kind)


def setup_inputs(seed: int = 0) -> dict:
    streams_of = jax.random.split(jax.random.key(seed), 17)
    pool_states = normal_values(streams_of[0], (POOL_SLOTS, HEAD_COUNT, HEAD_DIM, STATE_DIM), 1.0, 6.0, ((0, 8), (1, 4)), jnp.float32)
    inner_window = normal_values(streams_of[1], (POOL_SLOTS, KERNEL - 1, INNER_DIM), 1.0, 6.0, ((0, 8), (2, 4)))
    state_window = normal_values(streams_of[2], (POOL_SLOTS, KERNEL - 1, 2 * STATE_DIM), 1.0, 6.0, ((0, 8), (2, 4)))
    move_plan = draw_move_plan(jax.random.fold_in(streams_of[16], 71), 0)
    active_mask = plant((jax.random.randint(streams_of[4], (POOL_SLOTS,), 0, 4) < 3).astype(jnp.int32), jax.random.fold_in(streams_of[4], 1), 0, 1)
    inputs_inner = normal_values(streams_of[5], (PROMPT_TOTAL, PROMPT_SPAN, INNER_DIM), 1.0, 6.0, ((0, 8), (1, 4)))
    inputs_state = normal_values(streams_of[6], (PROMPT_TOTAL, PROMPT_SPAN, 2 * STATE_DIM), 1.0, 6.0, ((0, 8), (1, 4)))
    gate_rows = normal_values(streams_of[7], (PROMPT_TOTAL, PROMPT_SPAN, INNER_DIM), 1.0, 6.0, ((0, 8), (1, 4)))
    step_raw = draw_step_raw(jax.random.fold_in(streams_of[16], 71), 0)
    lengths = plant(jax.random.randint(streams_of[9], (PROMPT_TOTAL,), KERNEL, PROMPT_SPAN + 1), jax.random.fold_in(streams_of[9], 1), KERNEL, PROMPT_SPAN).astype(jnp.int32)
    conv_weight = normal_values(streams_of[10], (KERNEL, CHANNELS), KERNEL ** -0.5, 3.0, (), jnp.float32)
    conv_bias = normal_values(streams_of[11], (CHANNELS,), 0.5, 3.0, (), jnp.float32)
    step_bias = jnp.clip(jax.random.uniform(streams_of[12], (HEAD_COUNT,), jnp.float32, -3.3, -2.7), -3.3, -2.7)
    decay_log = draw_decay_log(jax.random.fold_in(streams_of[16], 71), 0)
    skip_weight = jnp.clip(jax.random.uniform(streams_of[14], (HEAD_COUNT,), jnp.float32, 0.5, 1.5), 0.5, 1.5)
    norm_weight = jnp.clip(1.0 + 0.15 * jax.random.normal(streams_of[15], (INNER_DIM,), jnp.float32), 0.25, 1.75)
    return dict(pool_states=pool_states, inner_window=inner_window, state_window=state_window, move_plan=move_plan, active_mask=active_mask, inputs_inner=inputs_inner, inputs_state=inputs_state, gate_rows=gate_rows, step_raw=step_raw, lengths=lengths, conv_weight=conv_weight, conv_bias=conv_bias, step_bias=step_bias, decay_log=decay_log, skip_weight=skip_weight, norm_weight=norm_weight)


EPSILON = 1e-05

def conv_silu(window, new_rows, weight, bias_values):
    extended = jnp.concatenate([window, new_rows], axis=1).astype(jnp.float32)
    length = new_rows.shape[1]
    running = jnp.zeros(new_rows.shape, jnp.float32) + bias_values
    for offset in range(weight.shape[0]):
        running = running + weight[offset] * extended[:, offset:offset + length]
    return jax.nn.silu(running).astype(jnp.bfloat16)

def block_local(value_rows, write_rows, read_rows, step_rows, decay_rates):
    log_decay = step_rows * decay_rates
    running_log = jnp.cumsum(log_decay, axis=0)
    scores = jnp.dot(read_rows, write_rows.T, preferred_element_type=jnp.float32)
    log_heads = running_log.T
    log_gaps = log_heads[:, :, None] - log_heads[:, None, :]
    positions = jnp.arange(running_log.shape[0])
    causal = positions[:, None] >= positions[None, :]
    decays = jnp.where(causal, jnp.exp(jnp.where(causal, log_gaps, 0.0)), 0.0)
    weights = (scores[None] * decays * step_rows.T[:, None, :]).astype(jnp.bfloat16)
    intra_part = jnp.einsum('hts,shp->thp', weights.astype(jnp.float32), value_rows.astype(jnp.float32))
    to_end = jnp.exp(running_log[-1:] - running_log) * step_rows
    scaled = (to_end[:, :, None] * value_rows.astype(jnp.float32)).astype(jnp.bfloat16)
    block_state = jnp.einsum('shp,sn->hpn', scaled.astype(jnp.float32), write_rows.astype(jnp.float32))
    return (intra_part, block_state, running_log)

def gated_norm(payload_array, gate_part, norm_weight):
    gated_rows = payload_array.astype(jnp.float32) * jax.nn.silu(gate_part.astype(jnp.float32))
    norm_scale = lax.rsqrt(lax.optimization_barrier(jnp.mean(gated_rows * gated_rows, axis=-1, keepdims=True)) + EPSILON)
    return (gated_rows * norm_scale * norm_weight).astype(jnp.bfloat16)

def reference(pool_states, inner_window, state_window, move_plan, active_mask, inputs_inner, inputs_state, gate_rows, step_raw, lengths, conv_weight, conv_bias, step_bias, decay_log, skip_weight, norm_weight):
    keep_flag = active_mask.astype(jnp.float32)
    targets = (move_plan[:, 0] * SLOTS_DEV + move_plan[:, 1]).astype(jnp.int32)
    moved_states = jnp.zeros_like(pool_states).at[targets].set(pool_states * keep_flag[:, None, None, None])
    moved_inner = jnp.zeros_like(inner_window).at[targets].set((inner_window.astype(jnp.float32) * keep_flag[:, None, None]).astype(jnp.bfloat16))
    moved_outer = jnp.zeros_like(state_window).at[targets].set((state_window.astype(jnp.float32) * keep_flag[:, None, None]).astype(jnp.bfloat16))
    sequence_index = jnp.arange(PROMPT_TOTAL).astype(jnp.int32)
    slot_index = (sequence_index // PREFILLS * SLOTS_DEV + sequence_index % PREFILLS).astype(jnp.int32)
    decay_rates = -jnp.exp(decay_log)
    block_count = PROMPT_SPAN // BLOCK_LEN

    def split_blocks(source):
        return source.reshape((block_count, BLOCK_LEN) + source.shape[1:])

    def one_block(members):
        return block_local(members[0], members[1], members[2], members[3], decay_rates)

    def advance(carried, members):
        block_state, running_log, read_block = members
        inter_part = jnp.einsum('qn,hpn->qhp', read_block.astype(jnp.float32), carried, precision=lax.Precision.HIGHEST) * jnp.exp(running_log)[:, :, None]
        updated = jnp.exp(running_log[-1])[:, None, None] * carried + block_state
        return (updated, inter_part)

    def prefill_one(members):
        initial, head_inner, head_outer, inner_rows, outer_rows, gate_part, step_part, length_one = members
        raw_rows = jnp.concatenate([inner_rows, outer_rows], axis=1)
        window = jnp.concatenate([head_inner, head_outer], axis=1)
        mixed_rows = conv_silu(window[None], raw_rows[None], conv_weight, conv_bias)[0]
        value_rows = mixed_rows[:, :INNER_DIM].reshape(PROMPT_SPAN, HEAD_COUNT, HEAD_DIM)
        write_rows = mixed_rows[:, INNER_DIM:INNER_DIM + STATE_DIM]
        read_rows = mixed_rows[:, INNER_DIM + STATE_DIM:]
        valid_rows = (jnp.arange(PROMPT_SPAN).astype(jnp.int32) < length_one).astype(jnp.float32)
        step_sizes = jax.nn.softplus(step_part.astype(jnp.float32) + step_bias) * valid_rows[:, None]
        intra_part, block_states, running_logs = lax.map(one_block, (split_blocks(value_rows), split_blocks(write_rows), split_blocks(read_rows), split_blocks(step_sizes)))
        final_state, inter_parts = lax.scan(advance, initial, (block_states, running_logs, split_blocks(read_rows)))
        combined = (intra_part + inter_parts).reshape(PROMPT_SPAN, HEAD_COUNT, HEAD_DIM) + skip_weight[:, None] * value_rows.astype(jnp.float32)
        y_rows = (combined * valid_rows[:, None, None]).astype(jnp.bfloat16).reshape(PROMPT_SPAN, INNER_DIM)
        mixer_rows = gated_norm(y_rows, gate_part, norm_weight)
        window_pos = (length_one - (KERNEL - 1) + jnp.arange(KERNEL - 1)).astype(jnp.int32)
        last_window = jnp.take(raw_rows, window_pos, axis=0)
        return (final_state, last_window, mixer_rows)
    final_states, last_windows, mixer_out = lax.map(prefill_one, (moved_states[slot_index], moved_inner[slot_index], moved_outer[slot_index], inputs_inner, inputs_state, gate_rows, step_raw, lengths))
    new_states = moved_states.at[slot_index].set(final_states)
    new_inner = moved_inner.at[slot_index].set(last_windows[:, :, :INNER_DIM])
    new_outer = moved_outer.at[slot_index].set(last_windows[:, :, INNER_DIM:])
    return (new_states, new_inner, new_outer, mixer_out)
```

```python
import functools

import jax
import jax.numpy as jnp
from jax import lax
from jax.experimental import pallas as pl
from jax.experimental.pallas import tpu as pltpu
from jax.sharding import PartitionSpec as P

HEAD_DIM = 64
STATE_DIM = 128
KERNEL = 4
BLOCK_LEN = 256
PREFILLS = 1
INNER_DIM = 4096


EPSILON = 1e-05


def shifted(value, axis, steps):
    count = lax.axis_size(axis)
    leading, last = (max(0, -steps), min(count, count - steps))
    return lax.ppermute(value, axis, [(source, source + steps) for source in range(leading, last)])


def entering(shard, axis, combine, identity):
    peers, index = (lax.axis_size(axis), lax.axis_index(axis))
    everything = jax.tree.map(lambda part: lax.all_gather(part, axis), shard)
    start = jax.tree.map(
        lambda part, zero: jnp.broadcast_to(jnp.asarray(zero, part.dtype), part.shape),
        shard,
        identity,
    )

    def hop(k, before):
        reached = k < index
        new = combine(before, jax.tree.map(lambda part: part[k], everything))
        return jax.tree.map(lambda a, b: jnp.where(reached, a, b), new, before)

    return lax.fori_loop(0, peers, hop, start)


def conv_silu(window, new_rows, weight, bias_values):
    extended = jnp.concatenate([window, new_rows], axis=1).astype(jnp.float32)
    length = new_rows.shape[1]
    running = jnp.zeros(new_rows.shape, jnp.float32) + bias_values
    for offset in range(weight.shape[0]):
        running = running + weight[offset] * extended[:, offset : offset + length]
    return jax.nn.silu(running).astype(jnp.bfloat16)


def block_local(value_rows, write_rows, read_rows, step_rows, decay_rates):
    log_decay = step_rows * decay_rates
    running_log = jnp.cumsum(log_decay, axis=0)
    scores = lax.dot_general(
        read_rows, write_rows, (((1,), (1,)), ((), ())), preferred_element_type=jnp.float32
    )
    log_heads = running_log.T
    log_gaps = log_heads[:, :, None] - log_heads[:, None, :]
    positions = jnp.arange(running_log.shape[0])
    causal = positions[:, None] >= positions[None, :]
    decays = jnp.where(causal, jnp.exp(jnp.where(causal, log_gaps, 0.0)), 0.0)
    weights = (scores[None] * decays * step_rows.T[:, None, :]).astype(jnp.bfloat16)
    intra_part = jnp.einsum("hts,shp->thp", weights, value_rows, preferred_element_type=jnp.float32)
    to_end = jnp.exp(running_log[-1:] - running_log) * step_rows
    scaled = (to_end[:, :, None] * value_rows.astype(jnp.float32)).astype(jnp.bfloat16)
    block_state = jnp.einsum("shp,sn->hpn", scaled, write_rows, preferred_element_type=jnp.float32)
    return (intra_part, block_state, running_log)


def local_parts(value_rows, write_rows, read_rows, step_rows, decay_rates):
    batch_size = value_rows.shape[0]
    block_count = value_rows.shape[1] // BLOCK_LEN

    def to_items(source):
        return source.reshape((batch_size * block_count, BLOCK_LEN) + source.shape[2:])

    def from_items(source):
        return source.reshape((batch_size, block_count) + source.shape[1:])

    def one_item(pieces):
        return block_local(pieces[0], pieces[1], pieces[2], pieces[3], decay_rates)

    results = lax.map(
        one_item,
        (to_items(value_rows), to_items(write_rows), to_items(read_rows), to_items(step_rows)),
    )
    return tuple((from_items(result) for result in results))


def blocked(source):
    return source.reshape(
        (source.shape[0], source.shape[1] // BLOCK_LEN, BLOCK_LEN) + source.shape[2:]
    )


def fold_states(initial, block_states, running_logs):

    def fold_advance(carried, pieces):
        return (jnp.exp(pieces[1][:, -1])[:, :, None, None] * carried + pieces[0], None)

    final_state, unused = lax.scan(
        fold_advance, initial, (jnp.moveaxis(block_states, 1, 0), jnp.moveaxis(running_logs, 1, 0))
    )
    return final_state


def run_states(initial, block_states, running_logs, read_blocks):

    def run_advance(carried, pieces):
        block_state, running_log, read_block = pieces
        inter_part = (
            jnp.einsum(
                "bqn,bhpn->bqhp",
                read_block.astype(jnp.float32),
                carried,
                precision=lax.Precision.HIGHEST,
            )
            * jnp.exp(running_log)[:, :, :, None]
        )
        updated = jnp.exp(running_log[:, -1])[:, :, None, None] * carried + block_state
        return (updated, inter_part)

    final_state, inter_parts = lax.scan(
        run_advance,
        initial,
        (
            jnp.moveaxis(block_states, 1, 0),
            jnp.moveaxis(running_logs, 1, 0),
            jnp.moveaxis(read_blocks, 1, 0),
        ),
    )
    return (final_state, jnp.moveaxis(inter_parts, 0, 1))


def assemble(intra_part, inter_parts, value_rows, skip_own, valid_rows):
    combined = (intra_part + inter_parts).reshape(value_rows.shape) + skip_own[
        :, None
    ] * value_rows.astype(jnp.float32)
    combined = combined * valid_rows[:, :, None, None]
    return combined.astype(jnp.bfloat16).reshape(value_rows.shape[0], value_rows.shape[1], -1)


def gated_norm(payload_array, gate_part, norm_weight):
    gated_rows = payload_array.astype(jnp.float32) * jax.nn.silu(gate_part.astype(jnp.float32))
    norm_scale = lax.rsqrt(jnp.mean(gated_rows * gated_rows, axis=-1, keepdims=True) + EPSILON)
    return (gated_rows * norm_scale * norm_weight).astype(jnp.bfloat16)


def last_rows(raw_rows, positions):

    def pick_rows(source_rows, indices):
        return jnp.take(source_rows, indices, axis=0)

    return jax.vmap(pick_rows)(raw_rows, positions)


def pack_kernel(source_ref, keep_ref, state_ref, out_ref):
    keep = keep_ref[pl.program_id(0)].astype(jnp.float32)
    out_ref[...] = (state_ref[...] * keep).astype(out_ref.dtype)


def pack_states(states, source_slot, keep):
    count = source_slot.shape[0]
    rows, lanes = states.shape[1:]
    return pl.pallas_call(
        pack_kernel,
        grid_spec=pltpu.PrefetchScalarGridSpec(
            num_scalar_prefetch=2,
            grid=(count,),
            in_specs=[pl.BlockSpec((1, rows, lanes), lambda i, source, keep: (source[i], 0, 0))],
            out_specs=pl.BlockSpec((1, rows, lanes), lambda i, source, keep: (i, 0, 0)),
        ),
        out_shape=jax.ShapeDtypeStruct((count, rows, lanes), jnp.bfloat16),
        compiler_params=pltpu.CompilerParams(dimension_semantics=("arbitrary",)),
        cost_estimate=pl.CostEstimate(
            flops=count * rows * lanes, bytes_accessed=6 * count * rows * lanes, transcendentals=0
        ),
    )(source_slot, keep, states)


def unpack_kernel(prefills, several, first_ref, later_ref, pick_ref, *refs):
    final_ref, head_ref = refs[:2]
    out_ref = refs[-1]
    slot = pl.program_id(0)

    @pl.when(slot < prefills)
    def _():
        out_ref[...] = final_ref[...]

    @pl.when((slot >= prefills) & (pick_ref[slot] == 0))
    def _():
        out_ref[...] = head_ref[...].astype(out_ref.dtype)

    if several:

        @pl.when((slot >= prefills) & (pick_ref[slot] != 0))
        def _():
            out_ref[...] = refs[2][...].astype(out_ref.dtype)


def unpack_states(final_own, head, rest, first, later, pick, slots):
    prefills, rows, lanes = final_own.shape
    block = (1, rows, lanes)
    several = rest is not None
    operands = [final_own, head] + ([rest] if several else [])
    in_specs = [
        pl.BlockSpec(block, lambda i, f, l, p: (jnp.minimum(i, prefills - 1), 0, 0)),
        pl.BlockSpec(block, lambda i, f, l, p: (f[i], 0, 0)),
    ]
    if several:
        in_specs.append(pl.BlockSpec(block, lambda i, f, l, p: (l[i], 0, 0)))
    return pl.pallas_call(
        functools.partial(unpack_kernel, prefills, several),
        grid_spec=pltpu.PrefetchScalarGridSpec(
            num_scalar_prefetch=3,
            grid=(slots,),
            in_specs=in_specs,
            out_specs=pl.BlockSpec(block, lambda i, f, l, p: (i, 0, 0)),
        ),
        out_shape=jax.ShapeDtypeStruct((slots, rows, lanes), jnp.float32),
        compiler_params=pltpu.CompilerParams(dimension_semantics=("arbitrary",)),
        cost_estimate=pl.CostEstimate(
            flops=slots * rows * lanes, bytes_accessed=6 * slots * rows * lanes, transcendentals=0
        ),
    )(first, later, pick, *operands)


def held_forward(indices, used):
    count = indices.shape[0]
    order = jnp.arange(count, dtype=jnp.int32)
    usable = used[None, :] & (order[None, :] <= order[:, None])
    last_used = jnp.max(jnp.where(usable, order[None, :], -1), axis=1)
    match = order[None, :] == last_used[:, None]
    return jnp.sum(jnp.where(match, indices[None, :], 0), axis=1).astype(jnp.int32)


def exchange(source):
    return lax.all_to_all(source, "req", split_axis=0, concat_axis=0, tiled=True)


def ranks_of(target_device, target_slot):
    slot_count = target_slot.shape[-1]
    slot_index = jnp.arange(slot_count, dtype=jnp.int32)
    order = jnp.where(target_slot < PREFILLS, slot_index, slot_index + slot_count)
    same = target_device[..., None, :] == target_device[..., :, None]
    earlier = same & (order[..., None, :] < order[..., :, None])
    return jnp.sum(earlier.astype(jnp.int32), axis=-1)


def migrate(pool_states, inner_window, state_window, move_plan, active_mask):
    slot_count = pool_states.shape[0]
    peer_count = lax.axis_size("req")
    capacity = (2 * slot_count + peer_count - 1) // peer_count
    keep_flag = active_mask.astype(jnp.float32)
    slot_index = jnp.arange(slot_count, dtype=jnp.int32)
    send_rank = ranks_of(move_plan[:, 0], move_plan[:, 1])
    peers = jnp.arange(peer_count)
    matches = (move_plan[:, 0][None, None, :] == peers[None, :, None]) & (
        send_rank[None, None, :] == jnp.arange(capacity)[:, None, None]
    )
    source_slot = jnp.sum(jnp.where(matches, slot_index[None, None, :], 0), axis=2)
    filled = jnp.any(matches, axis=2)
    every_plan = lax.all_gather(move_plan, "req")
    every_rank = ranks_of(every_plan[..., 0], every_plan[..., 1])
    mine = every_plan[..., 0] == lax.axis_index("req")
    hits = (mine[..., None] & (every_plan[..., 1][..., None] == slot_index)).astype(jnp.int32)
    from_peer = jnp.sum(hits * peers[:, None, None], axis=(0, 1)).astype(jnp.int32)
    from_rank = jnp.sum(hits * every_rank[..., None], axis=(0, 1)).astype(jnp.int32)

    windows = jnp.concatenate([inner_window, state_window], axis=2)
    windows = (windows.astype(jnp.float32) * keep_flag[:, None, None]).astype(jnp.bfloat16)
    send_windows = jnp.take(windows, source_slot.T.reshape(-1), axis=0)
    got_windows = exchange(send_windows.reshape((peer_count, capacity) + windows.shape[1:]))
    got_windows = got_windows.reshape((-1,) + windows.shape[1:])
    moved_windows = jnp.take(got_windows, from_peer * capacity + from_rank, axis=0)

    flat_states = pool_states.reshape(slot_count, -1, pool_states.shape[-1])

    def sent(low, high):
        part, used = source_slot[low:high].T.reshape(-1), filled[low:high].T.reshape(-1)
        keep = jnp.sum(
            jnp.where(part[:, None] == slot_index[None, :], active_mask[None, :], 0), axis=1
        )
        packed = pack_states(flat_states, held_forward(part, used), keep.astype(jnp.int32))
        return packed.reshape((peer_count, high - low) + packed.shape[1:])

    head = exchange(sent(0, 1)).reshape((peer_count,) + flat_states.shape[1:])
    rest = None
    if capacity > 1:
        later_send = sent(1, capacity)
        later_send, head = lax.optimization_barrier((later_send, head))
        rest = exchange(later_send).reshape((-1,) + flat_states.shape[1:])
    in_head = from_rank == 0
    first = held_forward(from_peer, in_head)
    later = held_forward(from_peer * max(1, capacity - 1) + from_rank - 1, ~in_head)
    pick = from_rank
    initial_own = lax.dynamic_index_in_dim(head, from_peer[0], 0, keepdims=True)
    initial_own = initial_own.astype(jnp.float32).reshape((PREFILLS,) + pool_states.shape[1:])
    inner_width = inner_window.shape[2]

    def place(final_own):
        final_rows = final_own.reshape((PREFILLS,) + flat_states.shape[1:])
        placed = unpack_states(final_rows, head, rest, first, later, pick, slot_count)
        return placed.reshape(pool_states.shape)

    return (
        initial_own,
        place,
        moved_windows[:, :, :inner_width],
        moved_windows[:, :, inner_width:],
    )


def combine_carries(earlier_part, later_part):
    return (
        earlier_part[0] * later_part[0],
        later_part[1] + later_part[0][:, :, None, None] * earlier_part[1],
    )


def on_device(
    pool_states,
    inner_window,
    state_window,
    move_plan,
    active_mask,
    inputs_inner,
    inputs_state,
    gate_rows,
    step_raw,
    lengths,
    conv_weight,
    conv_bias,
    step_bias,
    decay_log,
    skip_weight,
    norm_weight,
):
    initial_own, place, moved_inner, moved_outer = migrate(
        pool_states, inner_window, state_window, move_plan, active_mask
    )
    chain_index = lax.axis_index("seq")
    chain_size = lax.axis_size("seq")
    local_length = inputs_inner.shape[1]
    local_heads = initial_own.shape[1]
    decay_rates = -jnp.exp(decay_log)
    offsets = jnp.arange(KERNEL - 1, dtype=jnp.int32)
    raw_rows = jnp.concatenate([inputs_inner, inputs_state], axis=2)
    earlier_rows = shifted(raw_rows[:, local_length - KERNEL + 1 :], "seq", 1)
    initial, head_inner, head_outer = (
        lax.all_gather(initial_own, "seq", axis=1, tiled=True),
        lax.all_gather(moved_inner[:PREFILLS].astype(jnp.float32), "seq", axis=2, tiled=True),
        lax.all_gather(moved_outer[:PREFILLS].astype(jnp.float32), "seq", axis=2, tiled=True),
    )
    first_window = jnp.concatenate([head_inner, head_outer], axis=2).astype(jnp.bfloat16)
    window = jnp.where(chain_index == 0, first_window, earlier_rows)
    mixed_rows = conv_silu(window, raw_rows, conv_weight, conv_bias)
    positions = chain_index * local_length + jnp.arange(local_length, dtype=jnp.int32)
    valid_rows = (positions[None, :] < lengths[:, None]).astype(jnp.float32)
    step_sizes = jax.nn.softplus(step_raw.astype(jnp.float32) + step_bias) * valid_rows[:, :, None]
    value_rows = mixed_rows[:, :, :INNER_DIM].reshape(PREFILLS, local_length, -1, HEAD_DIM)
    write_rows = mixed_rows[:, :, INNER_DIM : INNER_DIM + STATE_DIM]
    read_rows = mixed_rows[:, :, INNER_DIM + STATE_DIM :]
    intra_part, block_states, running_logs = local_parts(
        value_rows, write_rows, read_rows, step_sizes, decay_rates
    )
    local_end = fold_states(jnp.zeros_like(block_states[:, 0]), block_states, running_logs)
    device_decay = jnp.exp(jnp.sum(step_sizes * decay_rates, axis=1))
    every_decay = lax.all_gather(device_decay[None], "seq", axis=0, tiled=True)
    prior_decay, prior_state = entering(
        (device_decay, local_end),
        "seq",
        combine_carries,
        (jnp.ones_like(device_decay), jnp.zeros_like(local_end)),
    )
    incoming = prior_state + prior_decay[:, :, None, None] * initial
    unused_final, inter_parts = run_states(incoming, block_states, running_logs, blocked(read_rows))
    later_mask = jnp.arange(chain_size)[:, None, None] > chain_index
    suffix = jnp.prod(jnp.where(later_mask, every_decay, 1.0), axis=0)
    whole_decay = jnp.prod(every_decay, axis=0)
    window_pos = lengths[:, None] - (KERNEL - 1) + offsets[None, :] - chain_index * local_length
    inside = ((window_pos >= 0) & (window_pos < local_length)).astype(jnp.float32)
    window_term = (
        last_rows(raw_rows, jnp.clip(window_pos, 0, local_length - 1)).astype(jnp.float32)
        * inside[:, :, None]
    )
    state_sum, inner_sum, outer_sum = (
        lax.psum_scatter(
            local_end * suffix[:, :, None, None], "seq", scatter_dimension=1, tiled=True
        ),
        lax.psum_scatter(window_term[:, :, :INNER_DIM], "seq", scatter_dimension=2, tiled=True),
        lax.psum_scatter(window_term[:, :, INNER_DIM:], "seq", scatter_dimension=2, tiled=True),
    )
    own_decay = lax.dynamic_slice_in_dim(whole_decay, chain_index * local_heads, local_heads, 1)
    final_own = state_sum + own_decay[:, :, None, None] * initial_own
    kept_inner = inner_sum.astype(jnp.bfloat16)
    kept_outer = outer_sum.astype(jnp.bfloat16)
    mixer_rows = assemble(intra_part, inter_parts, value_rows, skip_weight, valid_rows)
    mixer_out = gated_norm(mixer_rows, gate_rows, norm_weight)
    new_states = place(final_own)
    new_inner = jnp.concatenate([kept_inner, moved_inner[PREFILLS:]], axis=0)
    new_outer = jnp.concatenate([kept_outer, moved_outer[PREFILLS:]], axis=0)
    return (new_states, new_inner, new_outer, mixer_out)


def solution(mesh):
    return jax.shard_map(
        on_device,
        mesh=mesh,
        in_specs=(
            P("req", "seq", None, None),
            P("req", None, "seq"),
            P("req", None, "seq"),
            P("req", None),
            P("req"),
            P("req", "seq", None),
            P("req", "seq", None),
            P("req", "seq", None),
            P("req", "seq", None),
            P("req"),
            P(),
            P(),
            P(),
            P(),
            P(),
            P(),
        ),
        out_specs=(
            P("req", "seq", None, None),
            P("req", None, "seq"),
            P("req", None, "seq"),
            P("req", "seq", None),
        ),
        check_vma=False,
    )
```

```python
import functools

import jax
import jax.numpy as jnp
from jax import lax
from jax.experimental import pallas as pl
from jax.experimental.pallas import tpu as pltpu
from jax.sharding import PartitionSpec as P


HEAD_DIM = 64
STATE_DIM = 128
KERNEL = 4
BLOCK_LEN = 256
PREFILLS = 1
INNER_DIM = 4096


EPSILON = 1e-05


def shifted(value, axis, steps):
    count = lax.axis_size(axis)
    leading, last = (max(0, -steps), min(count, count - steps))
    return lax.ppermute(value, axis, [(source, source + steps) for source in range(leading, last)])


def entering(shard, axis, combine, identity):
    peers, index = (lax.axis_size(axis), lax.axis_index(axis))
    everything = jax.tree.map(lambda part: lax.all_gather(part, axis), shard)
    start = jax.tree.map(
        lambda part, zero: jnp.broadcast_to(jnp.asarray(zero, part.dtype), part.shape),
        shard,
        identity,
    )

    def hop(k, before):
        reached = k < index
        new = combine(before, jax.tree.map(lambda part: part[k], everything))
        return jax.tree.map(lambda a, b: jnp.where(reached, a, b), new, before)

    return lax.fori_loop(0, peers, hop, start)


def conv_silu(window, new_rows, weight, bias_values):
    extended = jnp.concatenate([window, new_rows], axis=1).astype(jnp.float32)
    length = new_rows.shape[1]
    running = jnp.zeros(new_rows.shape, jnp.float32) + bias_values
    for offset in range(weight.shape[0]):
        running = running + weight[offset] * extended[:, offset : offset + length]
    return jax.nn.silu(running).astype(jnp.bfloat16)


def block_local(value_rows, write_rows, read_rows, step_rows, decay_rates):
    log_decay = step_rows * decay_rates
    running_log = jnp.cumsum(log_decay, axis=0)
    scores = lax.dot_general(
        read_rows, write_rows, (((1,), (1,)), ((), ())), preferred_element_type=jnp.float32
    )
    log_heads = running_log.T
    log_gaps = log_heads[:, :, None] - log_heads[:, None, :]
    positions = jnp.arange(running_log.shape[0])
    causal = positions[:, None] >= positions[None, :]
    decays = jnp.where(causal, jnp.exp(jnp.where(causal, log_gaps, 0.0)), 0.0)
    weights = (scores[None] * decays * step_rows.T[:, None, :]).astype(jnp.bfloat16)
    intra_part = jnp.einsum("hts,shp->thp", weights, value_rows, preferred_element_type=jnp.float32)
    to_end = jnp.exp(running_log[-1:] - running_log) * step_rows
    scaled = (to_end[:, :, None] * value_rows.astype(jnp.float32)).astype(jnp.bfloat16)
    block_state = jnp.einsum("shp,sn->hpn", scaled, write_rows, preferred_element_type=jnp.float32)
    return (intra_part, block_state, running_log)


def local_parts(value_rows, write_rows, read_rows, step_rows, decay_rates):
    batch_size = value_rows.shape[0]
    block_count = value_rows.shape[1] // BLOCK_LEN

    def to_items(source):
        return source.reshape((batch_size * block_count, BLOCK_LEN) + source.shape[2:])

    def from_items(source):
        return source.reshape((batch_size, block_count) + source.shape[1:])

    def one_item(pieces):
        return block_local(pieces[0], pieces[1], pieces[2], pieces[3], decay_rates)

    results = lax.map(
        one_item,
        (to_items(value_rows), to_items(write_rows), to_items(read_rows), to_items(step_rows)),
    )
    return tuple((from_items(result) for result in results))


def blocked(source):
    return source.reshape(
        (source.shape[0], source.shape[1] // BLOCK_LEN, BLOCK_LEN) + source.shape[2:]
    )


def fold_states(initial, block_states, running_logs):

    def fold_advance(carried, pieces):
        return (jnp.exp(pieces[1][:, -1])[:, :, None, None] * carried + pieces[0], None)

    final_state, _ = lax.scan(
        fold_advance, initial, (jnp.moveaxis(block_states, 1, 0), jnp.moveaxis(running_logs, 1, 0))
    )
    return final_state


def run_states(initial, block_states, running_logs, read_blocks):

    def run_advance(carried, pieces):
        block_state, running_log, read_block = pieces
        inter_part = (
            jnp.einsum(
                "bqn,bhpn->bqhp",
                read_block.astype(jnp.float32),
                carried,
                precision=lax.Precision.HIGHEST,
            )
            * jnp.exp(running_log)[:, :, :, None]
        )
        updated = jnp.exp(running_log[:, -1])[:, :, None, None] * carried + block_state
        return (updated, inter_part)

    final_state, inter_parts = lax.scan(
        run_advance,
        initial,
        (
            jnp.moveaxis(block_states, 1, 0),
            jnp.moveaxis(running_logs, 1, 0),
            jnp.moveaxis(read_blocks, 1, 0),
        ),
    )
    return (final_state, jnp.moveaxis(inter_parts, 0, 1))


def assemble(intra_part, inter_parts, value_rows, skip_own, valid_rows):
    combined = (intra_part + inter_parts).reshape(value_rows.shape) + skip_own[
        :, None
    ] * value_rows.astype(jnp.float32)
    combined = combined * valid_rows[:, :, None, None]
    return combined.astype(jnp.bfloat16).reshape(value_rows.shape[0], value_rows.shape[1], -1)


def gated_norm(payload_array, gate_part, norm_weight):
    gated_rows = payload_array.astype(jnp.float32) * jax.nn.silu(gate_part.astype(jnp.float32))
    norm_scale = lax.rsqrt(jnp.mean(gated_rows * gated_rows, axis=-1, keepdims=True) + EPSILON)
    return (gated_rows * norm_scale * norm_weight).astype(jnp.bfloat16)


def last_rows(raw_rows, positions):

    def pick_rows(source_rows, indices):
        return jnp.take(source_rows, indices, axis=0)

    return jax.vmap(pick_rows)(raw_rows, positions)


def pack_kernel(source_ref, keep_ref, state_ref, out_ref):
    keep = keep_ref[pl.program_id(0)].astype(jnp.float32)
    out_ref[...] = (state_ref[...] * keep).astype(out_ref.dtype)


def pack_states(states, source_slot, keep):
    count = source_slot.shape[0]
    rows, lanes = states.shape[1:]
    return pl.pallas_call(
        pack_kernel,
        grid_spec=pltpu.PrefetchScalarGridSpec(
            num_scalar_prefetch=2,
            grid=(count,),
            in_specs=[pl.BlockSpec((1, rows, lanes), lambda i, source, keep: (source[i], 0, 0))],
            out_specs=pl.BlockSpec((1, rows, lanes), lambda i, source, keep: (i, 0, 0)),
        ),
        out_shape=jax.ShapeDtypeStruct((count, rows, lanes), jnp.bfloat16),
        compiler_params=pltpu.CompilerParams(dimension_semantics=("arbitrary",)),
        cost_estimate=pl.CostEstimate(
            flops=count * rows * lanes, bytes_accessed=6 * count * rows * lanes, transcendentals=0
        ),
    )(source_slot, keep, states)


def unpack_kernel(prefills, several, first_ref, later_ref, pick_ref, *refs):
    final_ref, head_ref = refs[:2]
    out_ref = refs[-1]
    slot = pl.program_id(0)

    @pl.when(slot < prefills)
    def _():
        out_ref[...] = final_ref[...]

    @pl.when((slot >= prefills) & (pick_ref[slot] == 0))
    def _():
        out_ref[...] = head_ref[...].astype(out_ref.dtype)

    if several:

        @pl.when((slot >= prefills) & (pick_ref[slot] != 0))
        def _():
            out_ref[...] = refs[2][...].astype(out_ref.dtype)


def unpack_states(final_own, head, rest, first, later, pick, slots):
    prefills, rows, lanes = final_own.shape
    block = (1, rows, lanes)
    several = rest is not None
    operands = [final_own, head] + ([rest] if several else [])
    in_specs = [
        pl.BlockSpec(block, lambda i, f, l, p: (jnp.minimum(i, prefills - 1), 0, 0)),
        pl.BlockSpec(block, lambda i, f, l, p: (f[i], 0, 0)),
    ]
    if several:
        in_specs.append(pl.BlockSpec(block, lambda i, f, l, p: (l[i], 0, 0)))
    return pl.pallas_call(
        functools.partial(unpack_kernel, prefills, several),
        grid_spec=pltpu.PrefetchScalarGridSpec(
            num_scalar_prefetch=3,
            grid=(slots,),
            in_specs=in_specs,
            out_specs=pl.BlockSpec(block, lambda i, f, l, p: (i, 0, 0)),
        ),
        out_shape=jax.ShapeDtypeStruct((slots, rows, lanes), jnp.float32),
        compiler_params=pltpu.CompilerParams(dimension_semantics=("arbitrary",)),
        cost_estimate=pl.CostEstimate(
            flops=slots * rows * lanes, bytes_accessed=6 * slots * rows * lanes, transcendentals=0
        ),
    )(first, later, pick, *operands)


def held_forward(indices, used):
    count = indices.shape[0]
    order = jnp.arange(count, dtype=jnp.int32)
    usable = used[None, :] & (order[None, :] <= order[:, None])
    last_used = jnp.max(jnp.where(usable, order[None, :], -1), axis=1)
    match = order[None, :] == last_used[:, None]
    return jnp.sum(jnp.where(match, indices[None, :], 0), axis=1).astype(jnp.int32)


def exchange(source):
    return lax.all_to_all(source, "req", split_axis=0, concat_axis=0, tiled=True)


def ranks_of(target_device, target_slot):
    slot_count = target_slot.shape[-1]
    slot_index = jnp.arange(slot_count, dtype=jnp.int32)
    order = jnp.where(target_slot < PREFILLS, slot_index, slot_index + slot_count)
    same = target_device[..., None, :] == target_device[..., :, None]
    earlier = same & (order[..., None, :] < order[..., :, None])
    return jnp.sum(earlier.astype(jnp.int32), axis=-1)


def migrate(pool_states, inner_window, state_window, move_plan, active_mask):
    slot_count = pool_states.shape[0]
    peer_count = lax.axis_size("req")
    capacity = (2 * slot_count + peer_count - 1) // peer_count
    keep_flag = active_mask.astype(jnp.float32)
    slot_index = jnp.arange(slot_count, dtype=jnp.int32)
    send_rank = ranks_of(move_plan[:, 0], move_plan[:, 1])
    peers = jnp.arange(peer_count)
    matches = (move_plan[:, 0][None, None, :] == peers[None, :, None]) & (
        send_rank[None, None, :] == jnp.arange(capacity)[:, None, None]
    )
    source_slot = jnp.sum(jnp.where(matches, slot_index[None, None, :], 0), axis=2)
    filled = jnp.any(matches, axis=2)
    every_plan = lax.all_gather(move_plan, "req")
    every_rank = ranks_of(every_plan[..., 0], every_plan[..., 1])
    mine = every_plan[..., 0] == lax.axis_index("req")
    hits = (mine[..., None] & (every_plan[..., 1][..., None] == slot_index)).astype(jnp.int32)
    from_peer = jnp.sum(hits * peers[:, None, None], axis=(0, 1)).astype(jnp.int32)
    from_rank = jnp.sum(hits * every_rank[..., None], axis=(0, 1)).astype(jnp.int32)

    windows = jnp.concatenate([inner_window, state_window], axis=2)
    windows = (windows.astype(jnp.float32) * keep_flag[:, None, None]).astype(jnp.bfloat16)
    send_windows = jnp.take(windows, source_slot.T.reshape(-1), axis=0)
    got_windows = exchange(send_windows.reshape((peer_count, capacity) + windows.shape[1:]))
    got_windows = got_windows.reshape((-1,) + windows.shape[1:])
    moved_windows = jnp.take(got_windows, from_peer * capacity + from_rank, axis=0)

    flat_states = pool_states.reshape(slot_count, -1, pool_states.shape[-1])

    def sent(low, high):
        part, used = source_slot[low:high].T.reshape(-1), filled[low:high].T.reshape(-1)
        keep = jnp.sum(
            jnp.where(part[:, None] == slot_index[None, :], active_mask[None, :], 0), axis=1
        )
        packed = pack_states(flat_states, held_forward(part, used), keep.astype(jnp.int32))
        return packed.reshape((peer_count, high - low) + packed.shape[1:])

    head_send = sent(0, 1)
    head = exchange(head_send)
    head = head.reshape((peer_count,) + flat_states.shape[1:])
    rest = None
    if capacity > 1:
        later_send = sent(1, capacity)
        later_send, head = lax.optimization_barrier((later_send, head))
        rest = exchange(later_send)
        rest = rest.reshape((-1,) + flat_states.shape[1:])
    in_head = from_rank == 0
    first = held_forward(from_peer, in_head)
    later = held_forward(from_peer * max(1, capacity - 1) + from_rank - 1, ~in_head)
    pick = from_rank
    initial_own = lax.dynamic_index_in_dim(head, from_peer[0], 0, keepdims=True)
    initial_own = initial_own.astype(jnp.float32).reshape((PREFILLS,) + pool_states.shape[1:])
    inner_width = inner_window.shape[2]

    def place(final_own):
        final_rows = final_own.reshape((PREFILLS,) + flat_states.shape[1:])
        placed = unpack_states(final_rows, head, rest, first, later, pick, slot_count)
        return placed.reshape(pool_states.shape)

    return (
        initial_own,
        place,
        moved_windows[:, :, :inner_width],
        moved_windows[:, :, inner_width:],
    )


def combine_carries(earlier_part, later_part):
    return (
        earlier_part[0] * later_part[0],
        later_part[1] + later_part[0][:, :, None, None] * earlier_part[1],
    )


def on_device(
    pool_states,
    inner_window,
    state_window,
    move_plan,
    active_mask,
    inputs_inner,
    inputs_state,
    gate_rows,
    step_raw,
    lengths,
    conv_weight,
    conv_bias,
    step_bias,
    decay_log,
    skip_weight,
    norm_weight,
):
    initial_own, place, moved_inner, moved_outer = migrate(
        pool_states, inner_window, state_window, move_plan, active_mask
    )
    chain_index = lax.axis_index("seq")
    chain_size = lax.axis_size("seq")
    local_length = inputs_inner.shape[1]
    local_heads = initial_own.shape[1]
    decay_rates = -jnp.exp(decay_log)
    offsets = jnp.arange(KERNEL - 1, dtype=jnp.int32)
    raw_rows = jnp.concatenate([inputs_inner, inputs_state], axis=2)
    earlier_rows = shifted(raw_rows[:, local_length - KERNEL + 1 :], "seq", 1)
    initial = lax.all_gather(initial_own, "seq", axis=1, tiled=True)
    head_inner, head_outer = (
        lax.all_gather(moved_inner[:PREFILLS].astype(jnp.float32), "seq", axis=2, tiled=True),
        lax.all_gather(moved_outer[:PREFILLS].astype(jnp.float32), "seq", axis=2, tiled=True),
    )
    first_window = jnp.concatenate([head_inner, head_outer], axis=2).astype(jnp.bfloat16)
    window = jnp.where(chain_index == 0, first_window, earlier_rows)
    mixed_rows = conv_silu(window, raw_rows, conv_weight, conv_bias)
    positions = chain_index * local_length + jnp.arange(local_length, dtype=jnp.int32)
    valid_rows = (positions[None, :] < lengths[:, None]).astype(jnp.float32)
    step_sizes = jax.nn.softplus(step_raw.astype(jnp.float32) + step_bias) * valid_rows[:, :, None]
    value_rows = mixed_rows[:, :, :INNER_DIM].reshape(PREFILLS, local_length, -1, HEAD_DIM)
    write_rows = mixed_rows[:, :, INNER_DIM : INNER_DIM + STATE_DIM]
    read_rows = mixed_rows[:, :, INNER_DIM + STATE_DIM :]
    intra_part, block_states, running_logs = local_parts(
        value_rows, write_rows, read_rows, step_sizes, decay_rates
    )
    local_end = fold_states(jnp.zeros_like(block_states[:, 0]), block_states, running_logs)
    device_decay = jnp.exp(jnp.sum(step_sizes * decay_rates, axis=1))
    device_decay, write_rows = lax.optimization_barrier((device_decay, write_rows))
    every_decay = lax.all_gather(device_decay[None], "seq", axis=0, tiled=True)
    prior_decay, prior_state = entering(
        (device_decay, local_end),
        "seq",
        combine_carries,
        (jnp.ones_like(device_decay), jnp.zeros_like(local_end)),
    )
    incoming = prior_state + prior_decay[:, :, None, None] * initial
    _, inter_parts = run_states(incoming, block_states, running_logs, blocked(read_rows))
    later_mask = jnp.arange(chain_size)[:, None, None] > chain_index
    suffix = jnp.prod(jnp.where(later_mask, every_decay, 1.0), axis=0)
    whole_decay = jnp.prod(every_decay, axis=0)
    window_pos = lengths[:, None] - (KERNEL - 1) + offsets[None, :] - chain_index * local_length
    inside = ((window_pos >= 0) & (window_pos < local_length)).astype(jnp.float32)
    window_term = (
        last_rows(raw_rows, jnp.clip(window_pos, 0, local_length - 1)).astype(jnp.float32)
        * inside[:, :, None]
    )
    state_sum, inner_sum, outer_sum = (
        lax.psum_scatter(
            local_end * suffix[:, :, None, None], "seq", scatter_dimension=1, tiled=True
        ),
        lax.psum_scatter(window_term[:, :, :INNER_DIM], "seq", scatter_dimension=2, tiled=True),
        lax.psum_scatter(window_term[:, :, INNER_DIM:], "seq", scatter_dimension=2, tiled=True),
    )
    own_decay = lax.dynamic_slice_in_dim(whole_decay, chain_index * local_heads, local_heads, 1)
    final_own = state_sum + own_decay[:, :, None, None] * initial_own
    kept_inner = inner_sum.astype(jnp.bfloat16)
    kept_outer = outer_sum.astype(jnp.bfloat16)
    mixer_rows = assemble(intra_part, inter_parts, value_rows, skip_weight, valid_rows)
    mixer_out = gated_norm(mixer_rows, gate_rows, norm_weight)
    new_states = place(final_own)
    new_inner = jnp.concatenate([kept_inner, moved_inner[PREFILLS:]], axis=0)
    new_outer = jnp.concatenate([kept_outer, moved_outer[PREFILLS:]], axis=0)
    return (new_states, new_inner, new_outer, mixer_out)


def solution(mesh):
    return jax.shard_map(
        on_device,
        mesh=mesh,
        in_specs=(
            P("req", "seq", None, None),
            P("req", None, "seq"),
            P("req", None, "seq"),
            P("req", None),
            P("req"),
            P("req", "seq", None),
            P("req", "seq", None),
            P("req", "seq", None),
            P("req", "seq", None),
            P("req"),
            P(),
            P(),
            P(),
            P(),
            P(),
            P(),
        ),
        out_specs=(
            P("req", "seq", None, None),
            P("req", None, "seq"),
            P("req", None, "seq"),
            P("req", "seq", None),
        ),
        check_vma=False,
    )
```
